32 devices in a mesh: dist: 4 (over y, core), pix: 8 (over z, x).
Axes of the slice: x: 2, y: 2, z: 4, core: 2. Of those that a mesh axis runs over, the one named last changes fastest.
Arguments:
- contrast: float32 [4, 2, 2048, 2048], P('dist', None, 'pix'), may hold values from -6 to 6
- defocus: float32 [4], P('dist'), may hold values from 40 to 400
- blurring: float32 [4], P('dist'), may hold values from 0.5 to 4
Outputs:
- phase: float32 [2, 2048, 2048], P(None, 'pix')
The draws below stay inside these ranges and needn't reach their ends.
All inputs are finite; a program needn't handle non-finite values.
Results may differ from the reference program's by a relative error of at most 0.0003.
Values sent between devices are 32-bit elements; how exact they have to be, the bound alone decides.
A program may use at most 64 MiB of HBM per device.

```python
import math
import jax
import jax.numpy as jnp
from jax import lax

NC = 2048
NR = 2048
PROJ = 2
NDIST = 4


def shard_levels(key, dims, cuts, least, high):
    def one(position, shards_of):
        steps = jax.random.uniform(jax.random.fold_in(jax.random.fold_in(key, 6), position), (shards_of,), jnp.float32, least / len(cuts), high / len(cuts))
        return jnp.repeat(jnp.exp(steps), dims[position] // shards_of).reshape((-1,) + (1,) * (len(dims) - position - 1))

    loudness = one(*cuts[0])
    for cut in cuts[1:]:
        loudness = loudness * one(*cut)
    return loudness


def bell_draw(stream_key, shape, deviation, most, shards=(), kind=jnp.bfloat16):
    result = deviation * jax.random.normal(stream_key, shape, jnp.float32)
    if shards:
        result = result * shard_levels(stream_key, shape, shards, -0.22, 0.18)
    return jnp.clip(result, -most, most).astype(kind)


def setup_inputs(seed: int = 0) -> dict:
    streams_of = jax.random.split(jax.random.key(seed), 4)
    return {
        "contrast": bell_draw(streams_of[0], (NDIST, PROJ, NR, NC), 1.0, 6.0, ((0, 4), (2, 8)), jnp.float32),
        "defocus": jnp.clip(jnp.exp(math.log(400.0) - 2.3025851 * jax.random.uniform(streams_of[1], (NDIST,), jnp.float32) ** shard_levels(streams_of[1], (NDIST,), ((0, 4),), -0.2, 0.2)), 40.0, 400.0),
        "blurring": jnp.clip(0.5 + 3.5 * jax.random.uniform(streams_of[2], (NDIST,), jnp.float32) ** shard_levels(streams_of[2], (NDIST,), ((0, 4),), -0.2, 0.2), 0.5, 4.0),
    }


ABSORB_RATIO = 0.1
REGULARIZER = 0.05


def signed_square(freq_index, period):
    shifted = freq_index - period * (2 * freq_index >= period).astype(jnp.int32)
    fraction = shifted.astype(jnp.float32) / period
    return fraction * fraction


def transfer(defocus_value, blur_rate, squared):
    return jnp.exp(-blur_rate * squared) * (jnp.sin(defocus_value * squared) + ABSORB_RATIO * jnp.cos(defocus_value * squared))


def reference(contrast, defocus, blurring):
    row_square = signed_square(jnp.arange(NR, dtype=jnp.int32), NR)
    col_square = signed_square(jnp.arange(NC, dtype=jnp.int32), NC)
    squared = row_square[:, None] + col_square[None, :]
    gain_table = transfer(defocus[:, None, None], blurring[:, None, None], squared[None])
    denominator = jnp.sum(gain_table * gain_table, axis=0) + REGULARIZER

    def one_window(window_index):
        images = lax.dynamic_index_in_dim(contrast, window_index, 1, keepdims=False)
        spectra = jnp.fft.fft2(images)
        numerator = jnp.sum(gain_table * spectra, axis=0)
        return jnp.real(jnp.fft.ifft2(numerator / (2.0 * denominator)))

    return lax.map(one_window, jnp.arange(PROJ, dtype=jnp.int32))
```

```python
import functools
import math

import jax
import jax.numpy as jnp
import numpy as np
from jax import lax
from jax.experimental import pallas as pl
from jax.experimental.pallas import tpu as pltpu
from jax.sharding import PartitionSpec as P

ABSORB_RATIO = 0.1
REGULARIZER = 0.05


def unit_phase(first_len, second_len, period):
    left_index = jnp.arange(first_len, dtype=jnp.int32)[:, None]
    right_index = jnp.arange(second_len, dtype=jnp.int32)[None, :]
    turn_count = left_index * right_index % period
    angles = 2.0 * math.pi / period * turn_count.astype(jnp.float32)
    return (jnp.cos(angles), -jnp.sin(angles))


def conjugate_flip(tables):
    return (tables[0], -tables[1])


def complex_product(pattern, real_part, imag_part, tables):
    cosine, sine_part = tables
    out_real = jnp.einsum(pattern, real_part, cosine, precision=lax.Precision.HIGHEST) - jnp.einsum(
        pattern, imag_part, sine_part, precision=lax.Precision.HIGHEST
    )
    out_imag = jnp.einsum(
        pattern, real_part, sine_part, precision=lax.Precision.HIGHEST
    ) + jnp.einsum(pattern, imag_part, cosine, precision=lax.Precision.HIGHEST)
    return (out_real, out_imag)


def apply_twist(real_part, imag_part, cosine, sine_part):
    return (real_part * cosine - imag_part * sine_part, real_part * sine_part + imag_part * cosine)


def signed_square(freq_index, period):
    shifted = freq_index - period * (2 * freq_index >= period).astype(jnp.int32)
    fraction = shifted.astype(jnp.float32) / period
    return fraction * fraction


def transfer(defocus_value, blur_rate, squared):
    return jnp.exp(-blur_rate * squared) * (
        jnp.sin(defocus_value * squared) + ABSORB_RATIO * jnp.cos(defocus_value * squared)
    )


def general_body(contrast, defocus, blurring):
    images = contrast[0]
    projections, rows_local, columns = images.shape
    pix_count = lax.axis_size("pix")
    col_block = columns // pix_count
    rows_total = rows_local * pix_count
    outer_table = unit_phase(col_block, col_block, col_block)
    pixel_lookup_table = unit_phase(pix_count, pix_count, pix_count)
    row_table = unit_phase(rows_local, rows_local, rows_local)
    col_twist = unit_phase(col_block, pix_count, columns)
    row_twist = unit_phase(rows_local, pix_count, rows_total)
    even_images = images[0::2]
    odd_images = images[1::2]
    shaped_real = even_images.reshape(projections // 2, rows_local, col_block, pix_count)
    shaped_imag = odd_images.reshape(projections // 2, rows_local, col_block, pix_count)
    section_real, section_imag = complex_product(
        "prbn,bc->pcrn", shaped_real, shaped_imag, outer_table
    )
    section_real, section_imag = apply_twist(
        section_real, section_imag, col_twist[0][:, None, :], col_twist[1][:, None, :]
    )
    spec_real, spec_imag = complex_product(
        "pcrn,nq->pcrq", section_real, section_imag, pixel_lookup_table
    )
    col_freq = col_block * lax.axis_index("pix") + jnp.arange(col_block, dtype=jnp.int32)
    row_freq = (
        pix_count * jnp.arange(rows_local, dtype=jnp.int32)[:, None]
        + jnp.arange(pix_count, dtype=jnp.int32)[None, :]
    )
    squared = (
        signed_square(row_freq, rows_total)[None, :, :]
        + signed_square(col_freq, columns)[:, None, None]
    )
    own_gain = transfer(defocus[0], blurring[0], squared)
    received_real = lax.all_to_all(spec_real, "pix", split_axis=3, concat_axis=3, tiled=True)
    received_imaginary = lax.all_to_all(spec_imag, "pix", split_axis=3, concat_axis=3, tiled=True)
    middle_real, middle_imaginary = complex_product(
        "uhqb,bn->uhqn", received_real, received_imaginary, pixel_lookup_table
    )
    middle_real, middle_imaginary = apply_twist(
        middle_real, middle_imaginary, row_twist[0], row_twist[1]
    )
    out_real, out_imag = complex_product("pcrk,rj->pcjk", middle_real, middle_imaginary, row_table)
    summands = (own_gain * out_real, own_gain * out_imag, (own_gain * own_gain)[None])
    totals = lax.psum((summands[0], summands[1], summands[2]), "dist")
    den_sum = totals[2][0]
    bottom = 2.0 * (den_sum + REGULARIZER)
    quot_real = totals[0] / bottom
    quot_imag = totals[1] / bottom
    backward_real, backward_imaginary = complex_product(
        "pcjk,rj->pcrk", quot_real, quot_imag, conjugate_flip(row_table)
    )
    backward_real, backward_imaginary = apply_twist(
        backward_real, backward_imaginary, row_twist[0], -row_twist[1]
    )
    backward_real, backward_imaginary = complex_product(
        "uotv,zv->uotz", backward_real, backward_imaginary, conjugate_flip(pixel_lookup_table)
    )
    backward_real = backward_real / rows_total
    backward_imaginary = backward_imaginary / rows_total
    twist_cos = col_twist[0]
    twist_sin = col_twist[1]
    received_real = lax.all_to_all(backward_real, "pix", split_axis=3, concat_axis=3, tiled=True)
    received_imaginary = lax.all_to_all(
        backward_imaginary, "pix", split_axis=3, concat_axis=3, tiled=True
    )
    middle_real, middle_imaginary = complex_product(
        "pcrq,nq->pcrn", received_real, received_imaginary, conjugate_flip(pixel_lookup_table)
    )
    cols_real, cols_imag = apply_twist(
        middle_real, middle_imaginary, twist_cos[:, None, :], -twist_sin[:, None, :]
    )
    phase_blocks = jnp.einsum(
        "pcrn,cb->prbn", cols_real, outer_table[0], precision=lax.Precision.HIGHEST
    ) + jnp.einsum("pcrn,cb->prbn", cols_imag, outer_table[1], precision=lax.Precision.HIGHEST)
    odd_blocks = jnp.einsum(
        "pcrn,cb->prbn", cols_imag, outer_table[0], precision=lax.Precision.HIGHEST
    ) - jnp.einsum("pcrn,cb->prbn", cols_real, outer_table[1], precision=lax.Precision.HIGHEST)
    paired_blocks = jnp.stack([phase_blocks, odd_blocks], axis=1)
    return (paired_blocks / columns).reshape(projections, rows_local, columns)


RADIX = 8
CHUNK = 16


def split_bf16(value):
    high = value.astype(jnp.bfloat16)
    return high, (value - high.astype(jnp.float32)).astype(jnp.bfloat16)


def split_table(table):
    high = table.astype(np.float32).astype(jnp.bfloat16)
    return high, (table - high.astype(np.float64)).astype(np.float32).astype(jnp.bfloat16)


def dot_nt(left, right):
    return lax.dot_general(left, right, (((1,), (1,)), ((), ())), preferred_element_type=jnp.float32)


def dot_nn(left, right):
    return lax.dot_general(left, right, (((1,), (0,)), ((), ())), preferred_element_type=jnp.float32)


def dot3(dot, left, right):
    return dot(left[0], right[0]) + (dot(left[0], right[1]) + dot(left[1], right[0]))


def small_dft(items, sign, turn, add, sub):
    count = len(items)
    if count == 1:
        return items
    even = small_dft(items[0::2], sign, turn, add, sub)
    odd = small_dft(items[1::2], sign, turn, add, sub)
    low, high = [], []
    for k in range(count // 2):
        moved = odd[k]
        if k:
            moved = turn(moved, k, count, sign)
        low.append(add(even[k], moved))
        high.append(sub(even[k], moved))
    return low + high


def pair_turn(item, k, count, sign):
    real, imag = item
    if 4 * k == count:
        return (-imag, real) if sign > 0 else (imag, -real)
    angle = sign * 2.0 * math.pi * k / count
    cosine, sine = math.cos(angle), math.sin(angle)
    return (real * cosine - imag * sine, real * sine + imag * cosine)


def pair_add(a, b):
    return (a[0] + b[0], a[1] + b[1])


def pair_sub(a, b):
    return (a[0] - b[0], a[1] - b[1])


pair_dft = functools.partial(small_dft, turn=pair_turn, add=pair_add, sub=pair_sub)


def col_forward_kernel(x_ref, th_ref, tl_ref, tw_ref, out_ref, yh_ref, yl_ref):
    _, rows, columns = x_ref.shape
    block = columns // RADIX
    per_q, _, width, _ = out_ref.shape[1:]

    def spread(i, carry):
        at = pl.ds(pl.multiple_of(i * CHUNK, CHUNK), CHUNK)
        parts = [
            (x_ref[0, at, j * block : (j + 1) * block], x_ref[1, at, j * block : (j + 1) * block])
            for j in range(RADIX)
        ]
        for q, (real, imag) in enumerate(pair_dft(parts, -1)):
            if q:
                cosine, sine = tw_ref[q, 0:1, :], tw_ref[q, 1:2, :]
                real, imag = real * cosine + imag * sine, imag * cosine - real * sine
            for half, value in enumerate((real, imag)):
                high, low = split_bf16(value)
                yh_ref[q, at, half * block : (half + 1) * block] = high
                yl_ref[q, at, half * block : (half + 1) * block] = low
        return carry

    lax.fori_loop(0, rows // CHUNK, spread, 0)

    def transform(q, carry):
        table = (th_ref[...], tl_ref[...])
        result = dot3(dot_nt, table, (yh_ref[q], yl_ref[q]))
        for part in range(per_q):
            for half in range(2):
                first = half * block + part * width
                out_ref[q, part, half] = result[first : first + width]
        return carry

    lax.fori_loop(0, RADIX, transform, 0)


def middle_kernel(scale, in_ref, th_ref, tl_ref, tw_ref, twc_ref, f_ref, g_ref, out_ref, yh_ref, yl_ref, t_ref):
    dists, pixes, _, width, block = in_ref.shape
    per_dist = width // CHUNK

    def spread(i, carry):
        dist = i // per_dist
        at = pl.ds(pl.multiple_of((i % per_dist) * CHUNK, CHUNK), CHUNK)
        to = pl.ds(pl.multiple_of(i * CHUNK, CHUNK), CHUNK)
        parts = [(in_ref[dist, j, 0, at, :], in_ref[dist, j, 1, at, :]) for j in range(pixes)]
        for q, (real, imag) in enumerate(pair_dft(parts, -1)):
            if q:
                cosine, sine = tw_ref[q, 0:1, :], tw_ref[q, 1:2, :]
                real, imag = real * cosine + imag * sine, imag * cosine - real * sine
            for half, value in enumerate((real, imag)):
                high, low = split_bf16(value)
                yh_ref[q, to, half * block : (half + 1) * block] = high
                yl_ref[q, to, half * block : (half + 1) * block] = low
        return carry

    lax.fori_loop(0, dists * per_dist, spread, 0)

    def transform(q, carry):
        table = (th_ref[...], tl_ref[...])
        spectrum = dot3(dot_nt, (yh_ref[q], yl_ref[q]), table)
        factors = f_ref[q]
        total_real = total_imag = bottom = None
        for dist in range(dists):
            gain = (
                factors[2 * dist : 2 * dist + 1] * g_ref[2 * dist]
                + factors[2 * dist + 1 : 2 * dist + 2] * g_ref[2 * dist + 1]
            )
            real = gain * spectrum[dist * width : (dist + 1) * width, :block]
            imag = gain * spectrum[dist * width : (dist + 1) * width, block:]
            square = gain * gain
            if dist == 0:
                total_real, total_imag, bottom = real, imag, square
            else:
                total_real, total_imag, bottom = total_real + real, total_imag + imag, bottom + square
        ratio = scale / (2.0 * (bottom + REGULARIZER))
        real, imag = total_real * ratio, total_imag * ratio
        stacked = jnp.concatenate(
            [jnp.concatenate([real, -imag], axis=1), jnp.concatenate([imag, real], axis=1)], axis=0
        )
        upper = (th_ref[:block, :], tl_ref[:block, :])
        t_ref[q] = dot3(dot_nt, upper, split_bf16(stacked))
        return carry

    lax.fori_loop(0, RADIX, transform, 0)

    lane = lax.broadcasted_iota(jnp.int32, (CHUNK, 2 * width), 1)
    flip = jnp.where(lane < width, -1.0, 1.0).astype(jnp.float32)

    def times_i(value):
        return pltpu.roll(value, width, 1) * flip

    def turn(value, k, count, sign):
        if 4 * k == count:
            return times_i(value)
        angle = sign * 2.0 * math.pi * k / count
        return value * math.cos(angle) + times_i(value) * math.sin(angle)

    def gather(i, carry):
        at = pl.ds(pl.multiple_of(i * CHUNK, CHUNK), CHUNK)
        twists = twc_ref[at, :]
        parts = []
        for q in range(RADIX):
            value = t_ref[q, at, :]
            if q:
                value = value * twists[:, q : q + 1] + times_i(value) * twists[:, RADIX + q : RADIX + q + 1]
            parts.append(value)
        done = small_dft(parts, 1, turn, lambda a, b: a + b, lambda a, b: a - b)
        for j in range(pixes):
            out_ref[j, at, :] = done[j]
        return carry

    lax.fori_loop(0, block // CHUNK, gather, 0)


def col_inverse_kernel(in_ref, th_ref, tl_ref, tw_ref, out_ref, ah_ref, al_ref, t_ref):
    _, per_q, rows, lanes = in_ref.shape
    block = per_q * lanes // 2
    for q in range(RADIX):
        for part in range(per_q):
            high, low = split_bf16(in_ref[q, part])
            ah_ref[q * rows : (q + 1) * rows, part * lanes : (part + 1) * lanes] = high
            al_ref[q * rows : (q + 1) * rows, part * lanes : (part + 1) * lanes] = low
    t_ref[...] = dot3(dot_nn, (ah_ref[...], al_ref[...]), (th_ref[...], tl_ref[...]))

    def gather(i, carry):
        at = pl.ds(pl.multiple_of(i * CHUNK, CHUNK), CHUNK)
        parts = []
        for q in range(RADIX):
            row = pl.ds(pl.multiple_of(q * rows + i * CHUNK, CHUNK), CHUNK)
            real, imag = t_ref[row, :block], t_ref[row, block:]
            if q:
                cosine, sine = tw_ref[q, 0:1, :], tw_ref[q, 1:2, :]
                real, imag = real * cosine - imag * sine, imag * cosine + real * sine
            parts.append((real, imag))
        for j, (real, imag) in enumerate(pair_dft(parts, 1)):
            out_ref[0, at, j * block : (j + 1) * block] = real
            out_ref[1, at, j * block : (j + 1) * block] = imag
        return carry

    lax.fori_loop(0, rows // CHUNK, gather, 0)


def exchange_kernel(dists, pixes, in_ref, out_ref, send_sem, recv_sem, own_sem):
    dist, pix = lax.axis_index("dist"), lax.axis_index("pix")
    count = dists * pixes
    me = dist * pixes + pix
    own = pltpu.make_async_copy(in_ref.at[me], out_ref.at[me], own_sem)
    own.start()

    def copy(step):
        target = (me + step) % count
        return pltpu.make_async_remote_copy(
            src_ref=in_ref.at[target],
            dst_ref=out_ref.at[me],
            send_sem=send_sem.at[step],
            recv_sem=recv_sem.at[step],
            device_id={"dist": target // pixes, "pix": target % pixes},
            device_id_type=pl.DeviceIdType.MESH,
        )

    def start(step, carry):
        copy(step).start()
        return carry

    def finish(step, carry):
        copy(step).wait_send()
        source = (me + count - step) % count
        pltpu.make_async_remote_copy(
            src_ref=in_ref.at[source],
            dst_ref=out_ref.at[source],
            send_sem=send_sem.at[step],
            recv_sem=recv_sem.at[step],
            device_id={"dist": source // pixes, "pix": source % pixes},
            device_id_type=pl.DeviceIdType.MESH,
        ).wait_recv()
        return carry

    lax.fori_loop(1, count, start, 0)
    lax.fori_loop(1, count, finish, 0)
    own.wait()


def exchange(dists, pixes, array):
    count = dists * pixes
    return pl.pallas_call(
        functools.partial(exchange_kernel, dists, pixes),
        out_shape=jax.ShapeDtypeStruct(array.shape, array.dtype),
        in_specs=[pl.BlockSpec(memory_space=pl.ANY)],
        out_specs=pl.BlockSpec(memory_space=pl.ANY),
        scratch_shapes=[
            pltpu.SemaphoreType.DMA((count,)),
            pltpu.SemaphoreType.DMA((count,)),
            pltpu.SemaphoreType.DMA,
        ],
        compiler_params=pltpu.CompilerParams(has_side_effects=True),
    )(array)


GATHER_PIECES = 4


def gather_kernel(in_ref, out_ref, sems, own_sem):
    dist = lax.axis_index("dist")
    rows = in_ref.shape[1]
    piece = rows // GATHER_PIECES
    mate = dist + 1 - 2 * (dist % 2)
    across = (dist + 2) % 4
    corner = (mate + 2) % 4

    def at(owner, c):
        return out_ref.at[:, pl.ds(pl.multiple_of(owner * rows + c * piece, piece), piece), :]

    def send(src, owner, c, kind, target):
        return pltpu.make_async_remote_copy(
            src_ref=src,
            dst_ref=at(owner, c),
            send_sem=sems.at[0, kind, c],
            recv_sem=sems.at[1, kind, c],
            device_id={"dist": target},
            device_id_type=pl.DeviceIdType.MESH,
        )

    def local(c):
        return in_ref.at[:, pl.ds(c * piece, piece), :]

    own = pltpu.make_async_copy(in_ref, out_ref.at[:, pl.ds(pl.multiple_of(dist * rows, rows), rows), :], own_sem)
    for c in range(GATHER_PIECES):
        send(local(c), dist, c, 0, across).start()
    for c in range(GATHER_PIECES):
        send(local(c), dist, c, 1, mate).start()
    own.start()
    for c in range(GATHER_PIECES):
        send(local(c), across, c, 0, across).wait_recv()
        send(at(across, c), across, c, 2, mate).start()
    for c in range(GATHER_PIECES):
        send(local(c), dist, c, 0, across).wait_send()
        send(local(c), mate, c, 1, mate).wait()
        send(at(across, c), across, c, 2, mate).wait_send()
        send(at(across, c), corner, c, 2, mate).wait_recv()
    own.wait()


def gather_dist(dists, array):
    pair, rows, columns = array.shape
    return pl.pallas_call(
        gather_kernel,
        out_shape=jax.ShapeDtypeStruct((pair, dists * rows, columns), array.dtype),
        in_specs=[pl.BlockSpec(memory_space=pl.ANY)],
        out_specs=pl.BlockSpec(memory_space=pl.ANY),
        scratch_shapes=[pltpu.SemaphoreType.DMA((2, 3, GATHER_PIECES)), pltpu.SemaphoreType.DMA],
        compiler_params=pltpu.CompilerParams(has_side_effects=True),
    )(array)


def freq_square(order, period):
    freq = RADIX * (order % (period // RADIX)) + order // (period // RADIX)
    return signed_square(freq, period)


def gain_factors(defocus, blurring, squared):
    envelope = jnp.exp(-blurring[:, None] * squared)
    sine = envelope * jnp.sin(defocus[:, None] * squared)
    cosine = envelope * jnp.cos(defocus[:, None] * squared)
    return sine, cosine


def vmem_call(kernel, out_shape, scratch, *args):
    return pl.pallas_call(
        kernel,
        out_shape=jax.ShapeDtypeStruct(out_shape, jnp.float32),
        in_specs=[pl.BlockSpec(memory_space=pltpu.VMEM)] * len(args),
        out_specs=pl.BlockSpec(memory_space=pltpu.VMEM),
        scratch_shapes=scratch,
    )(*args)


def fast_body(contrast, defocus, blurring):
    images = contrast[0]
    _, rows, columns = images.shape
    pixes, dists = lax.axis_size("pix"), lax.axis_size("dist")
    count = pixes * dists
    block = columns // RADIX
    width = columns // count
    per_q = block // width
    total_rows = rows * pixes
    out_rows = rows // dists

    turns = np.outer(np.arange(block), np.arange(block)) % block * (2.0 * np.pi / block)
    cosine, sine = np.cos(turns), np.sin(turns)
    table = np.block([[cosine, sine], [-sine, cosine]])
    order = np.concatenate(
        [np.arange(width) + part * width + half * block for part in range(per_q) for half in range(2)]
    )
    th, tl = split_table(table)
    ph, pl_ = split_table(table[order])
    twist = np.outer(np.arange(RADIX), np.arange(block)) * (2.0 * np.pi / columns)
    tw = np.stack([np.cos(twist), np.sin(twist)], axis=1).astype(np.float32)
    twc = np.concatenate([np.cos(twist).T, np.sin(twist).T], axis=1).astype(np.float32)

    both = lax.all_gather(jnp.concatenate([defocus, blurring]), "dist")
    defocus_all, blurring_all = both[:, 0], both[:, 1]
    row_sine, row_cosine = gain_factors(
        defocus_all, blurring_all, freq_square(jnp.arange(total_rows, dtype=jnp.int32), total_rows)[None]
    )
    me = lax.axis_index("dist") * pixes + lax.axis_index("pix")
    col_sine, col_cosine = gain_factors(
        defocus_all, blurring_all, freq_square(me * width + jnp.arange(width, dtype=jnp.int32), columns)[None]
    )
    f_table = jnp.stack([row_sine, row_cosine], axis=1).reshape(2 * dists, RADIX, rows).transpose(1, 0, 2)
    g_table = jnp.stack(
        [col_cosine - ABSORB_RATIO * col_sine, col_sine + ABSORB_RATIO * col_cosine], axis=1
    ).reshape(2 * dists, width, 1)
    g_table = jnp.broadcast_to(g_table, (2 * dists, width, rows))

    spectra = vmem_call(
        col_forward_kernel,
        (RADIX, per_q, 2, width, rows),
        [pltpu.VMEM((RADIX, rows, 2 * block), jnp.bfloat16)] * 2,
        images, th, tl, tw,
    )
    received = exchange(dists, pixes, spectra.reshape(count, 2, width, rows))
    back = vmem_call(
        functools.partial(middle_kernel, 1.0 / (total_rows * columns)),
        (pixes, rows, 2 * width),
        [pltpu.VMEM((RADIX, dists * width, 2 * rows), jnp.bfloat16)] * 2
        + [pltpu.VMEM((RADIX, rows, 2 * width), jnp.float32)],
        received.reshape(dists, pixes, 2, width, rows), th, tl, tw, twc, f_table, g_table,
    )
    back = back.reshape(pixes, dists, out_rows, 2 * width).transpose(1, 0, 2, 3)
    arrived = exchange(dists, pixes, back.reshape(count, out_rows, 2 * width))
    phase = vmem_call(
        col_inverse_kernel,
        (2, out_rows, columns),
        [pltpu.VMEM((RADIX * out_rows, 2 * block), jnp.bfloat16)] * 2
        + [pltpu.VMEM((RADIX * out_rows, 2 * block), jnp.float32)],
        arrived.reshape(RADIX, per_q, out_rows, 2 * width), ph, pl_, tw,
    )
    return gather_dist(dists, phase)


def body(contrast, defocus, blurring):
    _, projections, rows, columns = contrast.shape
    pixes, dists = lax.axis_size("pix"), lax.axis_size("dist")
    fits = (
        projections == 2
        and pixes == RADIX
        and dists == 4
        and rows * pixes == columns
        and columns % (dists * pixes * 64) == 0
        and columns // (dists * pixes) == rows // dists == 64
    )
    return (fast_body if fits else general_body)(contrast, defocus, blurring)


def solution(mesh):
    return jax.shard_map(
        body,
        mesh=mesh,
        in_specs=(P("dist", None, "pix", None), P("dist"), P("dist")),
        out_specs=P(None, "pix", None),
        check_vma=False,
    )
```

```python
import functools
import math

import jax
import jax.numpy as jnp
import numpy as np
from jax import lax
from jax.experimental import pallas as pl
from jax.experimental.pallas import tpu as pltpu
from jax.sharding import PartitionSpec as P

ABSORB_RATIO = 0.1
REGULARIZER = 0.05


def unit_phase(first_len, second_len, period):
    left_index = jnp.arange(first_len, dtype=jnp.int32)[:, None]
    right_index = jnp.arange(second_len, dtype=jnp.int32)[None, :]
    turn_count = left_index * right_index % period
    angles = 2.0 * math.pi / period * turn_count.astype(jnp.float32)
    return (jnp.cos(angles), -jnp.sin(angles))


def conjugate_flip(tables):
    return (tables[0], -tables[1])


def complex_product(pattern, real_part, imag_part, tables):
    cosine, sine_part = tables
    out_real = jnp.einsum(pattern, real_part, cosine, precision=lax.Precision.HIGHEST) - jnp.einsum(
        pattern, imag_part, sine_part, precision=lax.Precision.HIGHEST
    )
    out_imag = jnp.einsum(
        pattern, real_part, sine_part, precision=lax.Precision.HIGHEST
    ) + jnp.einsum(pattern, imag_part, cosine, precision=lax.Precision.HIGHEST)
    return (out_real, out_imag)


def apply_twist(real_part, imag_part, cosine, sine_part):
    return (real_part * cosine - imag_part * sine_part, real_part * sine_part + imag_part * cosine)


def signed_square(freq_index, period):
    shifted = freq_index - period * (2 * freq_index >= period).astype(jnp.int32)
    fraction = shifted.astype(jnp.float32) / period
    return fraction * fraction


def transfer(defocus_value, blur_rate, squared):
    return jnp.exp(-blur_rate * squared) * (
        jnp.sin(defocus_value * squared) + ABSORB_RATIO * jnp.cos(defocus_value * squared)
    )


def general_body(contrast, defocus, blurring):
    images = contrast[0]
    projections, rows_local, columns = images.shape
    pix_count = lax.axis_size("pix")
    col_block = columns // pix_count
    rows_total = rows_local * pix_count
    outer_table = unit_phase(col_block, col_block, col_block)
    pixel_lookup_table = unit_phase(pix_count, pix_count, pix_count)
    row_table = unit_phase(rows_local, rows_local, rows_local)
    col_twist = unit_phase(col_block, pix_count, columns)
    row_twist = unit_phase(rows_local, pix_count, rows_total)
    even_images = images[0::2]
    odd_images = images[1::2]
    shaped_real = even_images.reshape(projections // 2, rows_local, col_block, pix_count)
    shaped_imag = odd_images.reshape(projections // 2, rows_local, col_block, pix_count)
    section_real, section_imag = complex_product(
        "prbn,bc->pcrn", shaped_real, shaped_imag, outer_table
    )
    section_real, section_imag = apply_twist(
        section_real, section_imag, col_twist[0][:, None, :], col_twist[1][:, None, :]
    )
    spec_real, spec_imag = complex_product(
        "pcrn,nq->pcrq", section_real, section_imag, pixel_lookup_table
    )
    col_freq = col_block * lax.axis_index("pix") + jnp.arange(col_block, dtype=jnp.int32)
    row_freq = (
        pix_count * jnp.arange(rows_local, dtype=jnp.int32)[:, None]
        + jnp.arange(pix_count, dtype=jnp.int32)[None, :]
    )
    squared = (
        signed_square(row_freq, rows_total)[None, :, :]
        + signed_square(col_freq, columns)[:, None, None]
    )
    own_gain = transfer(defocus[0], blurring[0], squared)
    received_real = lax.all_to_all(spec_real, "pix", split_axis=3, concat_axis=3, tiled=True)
    received_imaginary = lax.all_to_all(spec_imag, "pix", split_axis=3, concat_axis=3, tiled=True)
    middle_real, middle_imaginary = complex_product(
        "uhqb,bn->uhqn", received_real, received_imaginary, pixel_lookup_table
    )
    middle_real, middle_imaginary = apply_twist(
        middle_real, middle_imaginary, row_twist[0], row_twist[1]
    )
    out_real, out_imag = complex_product("pcrk,rj->pcjk", middle_real, middle_imaginary, row_table)
    summands = (own_gain * out_real, own_gain * out_imag, (own_gain * own_gain)[None])
    totals = lax.psum((summands[0], summands[1], summands[2]), "dist")
    den_sum = totals[2][0]
    bottom = 2.0 * (den_sum + REGULARIZER)
    quot_real = totals[0] / bottom
    quot_imag = totals[1] / bottom
    backward_real, backward_imaginary = complex_product(
        "pcjk,rj->pcrk", quot_real, quot_imag, conjugate_flip(row_table)
    )
    backward_real, backward_imaginary = apply_twist(
        backward_real, backward_imaginary, row_twist[0], -row_twist[1]
    )
    backward_real, backward_imaginary = complex_product(
        "uotv,zv->uotz", backward_real, backward_imaginary, conjugate_flip(pixel_lookup_table)
    )
    backward_real = backward_real / rows_total
    backward_imaginary = backward_imaginary / rows_total
    twist_cos = col_twist[0]
    twist_sin = col_twist[1]
    received_real = lax.all_to_all(backward_real, "pix", split_axis=3, concat_axis=3, tiled=True)
    received_imaginary = lax.all_to_all(
        backward_imaginary, "pix", split_axis=3, concat_axis=3, tiled=True
    )
    middle_real, middle_imaginary = complex_product(
        "pcrq,nq->pcrn", received_real, received_imaginary, conjugate_flip(pixel_lookup_table)
    )
    cols_real, cols_imag = apply_twist(
        middle_real, middle_imaginary, twist_cos[:, None, :], -twist_sin[:, None, :]
    )
    phase_blocks = jnp.einsum(
        "pcrn,cb->prbn", cols_real, outer_table[0], precision=lax.Precision.HIGHEST
    ) + jnp.einsum("pcrn,cb->prbn", cols_imag, outer_table[1], precision=lax.Precision.HIGHEST)
    odd_blocks = jnp.einsum(
        "pcrn,cb->prbn", cols_imag, outer_table[0], precision=lax.Precision.HIGHEST
    ) - jnp.einsum("pcrn,cb->prbn", cols_real, outer_table[1], precision=lax.Precision.HIGHEST)
    paired_blocks = jnp.stack([phase_blocks, odd_blocks], axis=1)
    return (paired_blocks / columns).reshape(projections, rows_local, columns)


RADIX = 8
CHUNK = 16


def split_bf16(value):
    high = value.astype(jnp.bfloat16)
    return high, (value - high.astype(jnp.float32)).astype(jnp.bfloat16)


def split_table(table):
    high = table.astype(np.float32).astype(jnp.bfloat16)
    return high, (table - high.astype(np.float64)).astype(np.float32).astype(jnp.bfloat16)


def dot_nt(left, right):
    return lax.dot_general(left, right, (((1,), (1,)), ((), ())), preferred_element_type=jnp.float32)


def dot_nn(left, right):
    return lax.dot_general(left, right, (((1,), (0,)), ((), ())), preferred_element_type=jnp.float32)


def dot3(dot, left, right):
    return dot(left[0], right[0]) + (dot(left[0], right[1]) + dot(left[1], right[0]))


def small_dft(items, sign, turn, add, sub):
    count = len(items)
    if count == 1:
        return items
    even = small_dft(items[0::2], sign, turn, add, sub)
    odd = small_dft(items[1::2], sign, turn, add, sub)
    low, high = [], []
    for k in range(count // 2):
        moved = odd[k]
        if k:
            moved = turn(moved, k, count, sign)
        low.append(add(even[k], moved))
        high.append(sub(even[k], moved))
    return low + high


def pair_turn(item, k, count, sign):
    real, imag = item
    if 4 * k == count:
        return (-imag, real) if sign > 0 else (imag, -real)
    angle = sign * 2.0 * math.pi * k / count
    cosine, sine = math.cos(angle), math.sin(angle)
    return (real * cosine - imag * sine, real * sine + imag * cosine)


def pair_add(a, b):
    return (a[0] + b[0], a[1] + b[1])


def pair_sub(a, b):
    return (a[0] - b[0], a[1] - b[1])


pair_dft = functools.partial(small_dft, turn=pair_turn, add=pair_add, sub=pair_sub)


def col_forward_kernel(x_ref, th_ref, tl_ref, tw_ref, out_ref, yh_ref, yl_ref):
    _, rows, columns = x_ref.shape
    block = columns // RADIX
    per_q, _, width, _ = out_ref.shape[1:]

    def spread(i, carry):
        at = pl.ds(pl.multiple_of(i * CHUNK, CHUNK), CHUNK)
        parts = [
            (x_ref[0, at, j * block : (j + 1) * block], x_ref[1, at, j * block : (j + 1) * block])
            for j in range(RADIX)
        ]
        for q, (real, imag) in enumerate(pair_dft(parts, -1)):
            if q:
                cosine, sine = tw_ref[q, 0:1, :], tw_ref[q, 1:2, :]
                real, imag = real * cosine + imag * sine, imag * cosine - real * sine
            for half, value in enumerate((real, imag)):
                high, low = split_bf16(value)
                yh_ref[q, at, half * block : (half + 1) * block] = high
                yl_ref[q, at, half * block : (half + 1) * block] = low
        return carry

    lax.fori_loop(0, rows // CHUNK, spread, 0)

    def transform(q, carry):
        table = (th_ref[...], tl_ref[...])
        result = dot3(dot_nt, table, (yh_ref[q], yl_ref[q]))
        for part in range(per_q):
            for half in range(2):
                first = half * block + part * width
                out_ref[q, part, half] = result[first : first + width]
        return carry

    lax.fori_loop(0, RADIX, transform, 0)


def middle_kernel(scale, in_ref, th_ref, tl_ref, tw_ref, twc_ref, f_ref, g_ref, out_ref, yh_ref, yl_ref, t_ref):
    dists, pixes, _, width, block = in_ref.shape
    per_dist = width // CHUNK

    def spread(i, carry):
        dist = i // per_dist
        at = pl.ds(pl.multiple_of((i % per_dist) * CHUNK, CHUNK), CHUNK)
        to = pl.ds(pl.multiple_of(i * CHUNK, CHUNK), CHUNK)
        parts = [(in_ref[dist, j, 0, at, :], in_ref[dist, j, 1, at, :]) for j in range(pixes)]
        for q, (real, imag) in enumerate(pair_dft(parts, -1)):
            if q:
                cosine, sine = tw_ref[q, 0:1, :], tw_ref[q, 1:2, :]
                real, imag = real * cosine + imag * sine, imag * cosine - real * sine
            for half, value in enumerate((real, imag)):
                high, low = split_bf16(value)
                yh_ref[q, to, half * block : (half + 1) * block] = high
                yl_ref[q, to, half * block : (half + 1) * block] = low
        return carry

    lax.fori_loop(0, dists * per_dist, spread, 0)

    def transform(q, carry):
        table = (th_ref[...], tl_ref[...])
        spectrum = dot3(dot_nt, (yh_ref[q], yl_ref[q]), table)
        factors = f_ref[q]
        total_real = total_imag = bottom = None
        for dist in range(dists):
            gain = (
                factors[2 * dist : 2 * dist + 1] * g_ref[2 * dist]
                + factors[2 * dist + 1 : 2 * dist + 2] * g_ref[2 * dist + 1]
            )
            real = gain * spectrum[dist * width : (dist + 1) * width, :block]
            imag = gain * spectrum[dist * width : (dist + 1) * width, block:]
            square = gain * gain
            if dist == 0:
                total_real, total_imag, bottom = real, imag, square
            else:
                total_real, total_imag, bottom = total_real + real, total_imag + imag, bottom + square
        ratio = scale / (2.0 * (bottom + REGULARIZER))
        real, imag = total_real * ratio, total_imag * ratio
        stacked = jnp.concatenate(
            [jnp.concatenate([real, -imag], axis=1), jnp.concatenate([imag, real], axis=1)], axis=0
        )
        upper = (th_ref[:block, :], tl_ref[:block, :])
        t_ref[q] = dot3(dot_nt, upper, split_bf16(stacked))
        return carry

    lax.fori_loop(0, RADIX, transform, 0)

    lane = lax.broadcasted_iota(jnp.int32, (CHUNK, 2 * width), 1)
    flip = jnp.where(lane < width, -1.0, 1.0).astype(jnp.float32)

    def times_i(value):
        return pltpu.roll(value, width, 1) * flip

    def turn(value, k, count, sign):
        if 4 * k == count:
            return times_i(value)
        angle = sign * 2.0 * math.pi * k / count
        return value * math.cos(angle) + times_i(value) * math.sin(angle)

    def gather(i, carry):
        at = pl.ds(pl.multiple_of(i * CHUNK, CHUNK), CHUNK)
        twists = twc_ref[at, :]
        parts = []
        for q in range(RADIX):
            value = t_ref[q, at, :]
            if q:
                value = value * twists[:, q : q + 1] + times_i(value) * twists[:, RADIX + q : RADIX + q + 1]
            parts.append(value)
        done = small_dft(parts, 1, turn, lambda a, b: a + b, lambda a, b: a - b)
        for j in range(pixes):
            out_ref[j, at, :] = done[j]
        return carry

    lax.fori_loop(0, block // CHUNK, gather, 0)


def col_inverse_kernel(in_ref, th_ref, tl_ref, tw_ref, out_ref, ah_ref, al_ref, t_ref):
    _, per_q, rows, lanes = in_ref.shape
    block = per_q * lanes // 2

    def transform(q, carry):
        for part in range(per_q):
            high, low = split_bf16(in_ref[q, part])
            ah_ref[:, part * lanes : (part + 1) * lanes] = high
            al_ref[:, part * lanes : (part + 1) * lanes] = low
        t_ref[q] = dot3(dot_nn, (ah_ref[...], al_ref[...]), (th_ref[...], tl_ref[...]))
        return carry

    lax.fori_loop(0, RADIX, transform, 0)

    def gather(i, carry):
        at = pl.ds(pl.multiple_of(i * CHUNK, CHUNK), CHUNK)
        parts = []
        for q in range(RADIX):
            real, imag = t_ref[q, at, :block], t_ref[q, at, block:]
            if q:
                cosine, sine = tw_ref[q, 0:1, :], tw_ref[q, 1:2, :]
                real, imag = real * cosine - imag * sine, imag * cosine + real * sine
            parts.append((real, imag))
        for j, (real, imag) in enumerate(pair_dft(parts, 1)):
            out_ref[0, at, j * block : (j + 1) * block] = real
            out_ref[1, at, j * block : (j + 1) * block] = imag
        return carry

    lax.fori_loop(0, rows // CHUNK, gather, 0)


def local_copy_spec():
    return pl.BlockSpec(memory_space=pl.ANY)


def remote(src, dst, send_sem, recv_sem, device_id):
    return pltpu.make_async_remote_copy(
        src_ref=src,
        dst_ref=dst,
        send_sem=send_sem,
        recv_sem=recv_sem,
        device_id=device_id,
        device_id_type=pl.DeviceIdType.MESH,
    )


def gain_factors(defocus, rate, squared):
    envelope = jnp.exp(-rate * squared)
    angle = defocus * squared
    return envelope * jnp.sin(angle), envelope * jnp.cos(angle)


def exchange_kernel(
    dists, pixes, in_ref, own_ref, out_ref, f_ref, g_ref,
    held, send_sem, recv_sem, own_sem, small_send, small_recv, small_own,
):
    dist, pix = lax.axis_index("dist"), lax.axis_index("pix")
    count = dists * pixes
    me = dist * pixes + pix

    def small(step, slot):
        return remote(
            own_ref, held.at[slot], small_send.at[step], small_recv.at[step], {"dist": (dist + step) % dists}
        )

    for step in range(1, dists):
        small(step, dist).start()
    small_copy = pltpu.make_async_copy(own_ref, held.at[dist], small_own)
    small_copy.start()
    own = pltpu.make_async_copy(in_ref.at[me], out_ref.at[me], own_sem)
    own.start()

    def copy(step):
        target = (me + step) % count
        return remote(
            in_ref.at[target], out_ref.at[me], send_sem.at[step], recv_sem.at[step],
            {"dist": target // pixes, "pix": target % pixes},
        )

    def start(step, carry):
        copy(step).start()
        return carry

    def finish(step, carry):
        copy(step).wait_send()
        source = (me + count - step) % count
        remote(
            in_ref.at[source], out_ref.at[source], send_sem.at[step], recv_sem.at[step],
            {"dist": source // pixes, "pix": source % pixes},
        ).wait_recv()
        return carry

    lax.fori_loop(1, count, start, 0)

    for step in range(1, dists):
        small(step, dist).wait_send()
        small(step, (dist + dists - step) % dists).wait_recv()
    small_copy.wait()
    radix, _, block = f_ref.shape
    _, width, _ = g_ref.shape
    row_freq = radix * lax.broadcasted_iota(jnp.int32, (radix, block), 1) + lax.broadcasted_iota(
        jnp.int32, (radix, block), 0
    )
    row_squared = signed_square(row_freq, radix * block)
    first = me * width
    col_freq = radix * (first % block + lax.broadcasted_iota(jnp.int32, (width, block), 0)) + first // block
    col_squared = signed_square(col_freq, radix * block)
    for d in range(dists):
        defocus, rate = held[d, 0:1, 0:1], held[d, 1:2, 0:1]
        sine, cosine = gain_factors(defocus, rate, row_squared)
        f_ref[:, 2 * d, :] = sine
        f_ref[:, 2 * d + 1, :] = cosine
        sine, cosine = gain_factors(defocus, rate, col_squared)
        g_ref[2 * d] = cosine - ABSORB_RATIO * sine
        g_ref[2 * d + 1] = sine + ABSORB_RATIO * cosine

    lax.fori_loop(1, count, finish, 0)
    own.wait()


def exchange(dists, pixes, array, own):
    count = dists * pixes
    _, _, width, rows = array.shape
    return pl.pallas_call(
        functools.partial(exchange_kernel, dists, pixes),
        out_shape=(
            jax.ShapeDtypeStruct(array.shape, array.dtype),
            jax.ShapeDtypeStruct((RADIX, 2 * dists, rows), jnp.float32),
            jax.ShapeDtypeStruct((2 * dists, width, rows), jnp.float32),
        ),
        in_specs=[local_copy_spec(), pl.BlockSpec(memory_space=pltpu.VMEM)],
        out_specs=(local_copy_spec(),) + (pl.BlockSpec(memory_space=pltpu.VMEM),) * 2,
        scratch_shapes=[
            pltpu.VMEM((dists,) + own.shape, jnp.float32),
            pltpu.SemaphoreType.DMA((count,)),
            pltpu.SemaphoreType.DMA((count,)),
            pltpu.SemaphoreType.DMA,
            pltpu.SemaphoreType.DMA((dists,)),
            pltpu.SemaphoreType.DMA((dists,)),
            pltpu.SemaphoreType.DMA,
        ],
        compiler_params=pltpu.CompilerParams(has_side_effects=True),
    )(array, own)


RELAY_LAG = 1


def relay_kernel(pixes, in_ref, out_ref, send_sem, recv_sem, hop_send, hop_recv, own_sem):
    dist, pix = lax.axis_index("dist"), lax.axis_index("pix")
    mate = dist + 1 - 2 * (dist % 2)
    across = (dist + 2) % 4
    corner = (mate + 2) % 4

    def first(step, source):
        target = (pix + step) % pixes
        return remote(
            in_ref.at[target], out_ref.at[dist, source], send_sem.at[step], recv_sem.at[step], {"pix": target}
        )

    def source_of(step):
        return (pix + pixes - step) % pixes

    def hop(owner, step, kind, target):
        block = out_ref.at[owner, source_of(step)]
        return remote(block, block, hop_send.at[kind, step], hop_recv.at[kind, step], {"dist": target})

    own = pltpu.make_async_copy(in_ref.at[pix], out_ref.at[dist, pix], own_sem)
    own.start()
    for step in range(1, pixes):
        first(step, pix).start()

    def relay(step):
        hop(across, step, 0, across).wait_recv()
        hop(across, step, 2, mate).start()

    for step in range(pixes):
        if step == 0:
            own.wait()
        else:
            first(step, source_of(step)).wait_recv()
        hop(dist, step, 0, across).start()
        hop(dist, step, 1, mate).start()
        if step >= RELAY_LAG:
            relay(step - RELAY_LAG)
    for step in range(pixes - RELAY_LAG, pixes):
        relay(step)
    for step in range(pixes):
        if step:
            first(step, pix).wait_send()
        hop(dist, step, 0, across).wait_send()
        hop(dist, step, 1, mate).wait_send()
        hop(mate, step, 1, mate).wait_recv()
        hop(across, step, 2, mate).wait_send()
        hop(corner, step, 2, mate).wait_recv()


def relay_all(dists, pixes, array):
    return pl.pallas_call(
        functools.partial(relay_kernel, pixes),
        out_shape=jax.ShapeDtypeStruct((dists,) + array.shape, array.dtype),
        in_specs=[local_copy_spec()],
        out_specs=local_copy_spec(),
        scratch_shapes=[
            pltpu.SemaphoreType.DMA((pixes,)),
            pltpu.SemaphoreType.DMA((pixes,)),
            pltpu.SemaphoreType.DMA((3, pixes)),
            pltpu.SemaphoreType.DMA((3, pixes)),
            pltpu.SemaphoreType.DMA,
        ],
        compiler_params=pltpu.CompilerParams(has_side_effects=True),
    )(array)


def vmem_call(kernel, out_shape, scratch, *args):
    return pl.pallas_call(
        kernel,
        out_shape=jax.ShapeDtypeStruct(out_shape, jnp.float32),
        in_specs=[pl.BlockSpec(memory_space=pltpu.VMEM)] * len(args),
        out_specs=pl.BlockSpec(memory_space=pltpu.VMEM),
        scratch_shapes=scratch,
    )(*args)


def fast_body(contrast, defocus, blurring):
    images = contrast[0]
    _, rows, columns = images.shape
    pixes, dists = lax.axis_size("pix"), lax.axis_size("dist")
    count = pixes * dists
    block = columns // RADIX
    width = columns // count
    per_q = block // width
    total_rows = rows * pixes

    turns = np.outer(np.arange(block), np.arange(block)) % block * (2.0 * np.pi / block)
    cosine, sine = np.cos(turns), np.sin(turns)
    table = np.block([[cosine, sine], [-sine, cosine]])
    order = np.concatenate(
        [np.arange(width) + part * width + half * block for part in range(per_q) for half in range(2)]
    )
    th, tl = split_table(table)
    ph, pl_ = split_table(table[order])
    twist = np.outer(np.arange(RADIX), np.arange(block)) * (2.0 * np.pi / columns)
    tw = np.stack([np.cos(twist), np.sin(twist)], axis=1).astype(np.float32)
    twc = np.concatenate([np.cos(twist).T, np.sin(twist).T], axis=1).astype(np.float32)

    own = jnp.broadcast_to(jnp.concatenate([defocus, blurring] * 4)[:, None], (8, 128))

    spectra = vmem_call(
        col_forward_kernel,
        (RADIX, per_q, 2, width, rows),
        [pltpu.VMEM((RADIX, rows, 2 * block), jnp.bfloat16)] * 2,
        images, th, tl, tw,
    )
    received, f_table, g_table = exchange(dists, pixes, spectra.reshape(count, 2, width, rows), own)
    back = vmem_call(
        functools.partial(middle_kernel, 1.0 / (total_rows * columns)),
        (pixes, rows, 2 * width),
        [pltpu.VMEM((RADIX, dists * width, 2 * rows), jnp.bfloat16)] * 2
        + [pltpu.VMEM((RADIX, rows, 2 * width), jnp.float32)],
        received.reshape(dists, pixes, 2, width, rows), th, tl, tw, twc, f_table, g_table,
    )
    arrived = relay_all(dists, pixes, back)
    return vmem_call(
        col_inverse_kernel,
        (2, rows, columns),
        [pltpu.VMEM((rows, 2 * block), jnp.bfloat16)] * 2
        + [pltpu.VMEM((RADIX, rows, 2 * block), jnp.float32)],
        arrived.reshape(RADIX, per_q, rows, 2 * width), ph, pl_, tw,
    )


def body(contrast, defocus, blurring):
    _, projections, rows, columns = contrast.shape
    pixes, dists = lax.axis_size("pix"), lax.axis_size("dist")
    fits = (
        projections == 2
        and pixes == RADIX
        and dists == 4
        and rows * pixes == columns
        and columns % (dists * pixes * 64) == 0
        and columns // (dists * pixes) == rows // dists == 64
    )
    return (fast_body if fits else general_body)(contrast, defocus, blurring)


def solution(mesh):
    return jax.shard_map(
        body,
        mesh=mesh,
        in_specs=(P("dist", None, "pix", None), P("dist"), P("dist")),
        out_specs=P(None, "pix", None),
        check_vma=False,
    )
```

```python
import functools
import math

import jax
import jax.numpy as jnp
import numpy as np
from jax import lax
from jax.experimental import pallas as pl
from jax.experimental.pallas import tpu as pltpu
from jax.sharding import PartitionSpec as P

ABSORB_RATIO = 0.1
REGULARIZER = 0.05


def unit_phase(first_len, second_len, period):
    left_index = jnp.arange(first_len, dtype=jnp.int32)[:, None]
    right_index = jnp.arange(second_len, dtype=jnp.int32)[None, :]
    turn_count = left_index * right_index % period
    angles = 2.0 * math.pi / period * turn_count.astype(jnp.float32)
    return (jnp.cos(angles), -jnp.sin(angles))


def conjugate_flip(tables):
    return (tables[0], -tables[1])


def complex_product(pattern, real_part, imag_part, tables):
    cosine, sine_part = tables
    out_real = jnp.einsum(pattern, real_part, cosine, precision=lax.Precision.HIGHEST) - jnp.einsum(
        pattern, imag_part, sine_part, precision=lax.Precision.HIGHEST
    )
    out_imag = jnp.einsum(
        pattern, real_part, sine_part, precision=lax.Precision.HIGHEST
    ) + jnp.einsum(pattern, imag_part, cosine, precision=lax.Precision.HIGHEST)
    return (out_real, out_imag)


def apply_twist(real_part, imag_part, cosine, sine_part):
    return (real_part * cosine - imag_part * sine_part, real_part * sine_part + imag_part * cosine)


def signed_square(freq_index, period):
    shifted = freq_index - period * (2 * freq_index >= period).astype(jnp.int32)
    fraction = shifted.astype(jnp.float32) / period
    return fraction * fraction


def transfer(defocus_value, blur_rate, squared):
    return jnp.exp(-blur_rate * squared) * (
        jnp.sin(defocus_value * squared) + ABSORB_RATIO * jnp.cos(defocus_value * squared)
    )


def general_body(contrast, defocus, blurring):
    images = contrast[0]
    projections, rows_local, columns = images.shape
    pix_count = lax.axis_size("pix")
    col_block = columns // pix_count
    rows_total = rows_local * pix_count
    outer_table = unit_phase(col_block, col_block, col_block)
    pixel_lookup_table = unit_phase(pix_count, pix_count, pix_count)
    row_table = unit_phase(rows_local, rows_local, rows_local)
    col_twist = unit_phase(col_block, pix_count, columns)
    row_twist = unit_phase(rows_local, pix_count, rows_total)
    even_images = images[0::2]
    odd_images = images[1::2]
    shaped_real = even_images.reshape(projections // 2, rows_local, col_block, pix_count)
    shaped_imag = odd_images.reshape(projections // 2, rows_local, col_block, pix_count)
    section_real, section_imag = complex_product(
        "prbn,bc->pcrn", shaped_real, shaped_imag, outer_table
    )
    section_real, section_imag = apply_twist(
        section_real, section_imag, col_twist[0][:, None, :], col_twist[1][:, None, :]
    )
    spec_real, spec_imag = complex_product(
        "pcrn,nq->pcrq", section_real, section_imag, pixel_lookup_table
    )
    col_freq = col_block * lax.axis_index("pix") + jnp.arange(col_block, dtype=jnp.int32)
    row_freq = (
        pix_count * jnp.arange(rows_local, dtype=jnp.int32)[:, None]
        + jnp.arange(pix_count, dtype=jnp.int32)[None, :]
    )
    squared = (
        signed_square(row_freq, rows_total)[None, :, :]
        + signed_square(col_freq, columns)[:, None, None]
    )
    own_gain = transfer(defocus[0], blurring[0], squared)
    received_real = lax.all_to_all(spec_real, "pix", split_axis=3, concat_axis=3, tiled=True)
    received_imaginary = lax.all_to_all(spec_imag, "pix", split_axis=3, concat_axis=3, tiled=True)
    middle_real, middle_imaginary = complex_product(
        "uhqb,bn->uhqn", received_real, received_imaginary, pixel_lookup_table
    )
    middle_real, middle_imaginary = apply_twist(
        middle_real, middle_imaginary, row_twist[0], row_twist[1]
    )
    out_real, out_imag = complex_product("pcrk,rj->pcjk", middle_real, middle_imaginary, row_table)
    summands = (own_gain * out_real, own_gain * out_imag, (own_gain * own_gain)[None])
    totals = lax.psum((summands[0], summands[1], summands[2]), "dist")
    den_sum = totals[2][0]
    bottom = 2.0 * (den_sum + REGULARIZER)
    quot_real = totals[0] / bottom
    quot_imag = totals[1] / bottom
    backward_real, backward_imaginary = complex_product(
        "pcjk,rj->pcrk", quot_real, quot_imag, conjugate_flip(row_table)
    )
    backward_real, backward_imaginary = apply_twist(
        backward_real, backward_imaginary, row_twist[0], -row_twist[1]
    )
    backward_real, backward_imaginary = complex_product(
        "uotv,zv->uotz", backward_real, backward_imaginary, conjugate_flip(pixel_lookup_table)
    )
    backward_real = backward_real / rows_total
    backward_imaginary = backward_imaginary / rows_total
    twist_cos = col_twist[0]
    twist_sin = col_twist[1]
    received_real = lax.all_to_all(backward_real, "pix", split_axis=3, concat_axis=3, tiled=True)
    received_imaginary = lax.all_to_all(
        backward_imaginary, "pix", split_axis=3, concat_axis=3, tiled=True
    )
    middle_real, middle_imaginary = complex_product(
        "pcrq,nq->pcrn", received_real, received_imaginary, conjugate_flip(pixel_lookup_table)
    )
    cols_real, cols_imag = apply_twist(
        middle_real, middle_imaginary, twist_cos[:, None, :], -twist_sin[:, None, :]
    )
    phase_blocks = jnp.einsum(
        "pcrn,cb->prbn", cols_real, outer_table[0], precision=lax.Precision.HIGHEST
    ) + jnp.einsum("pcrn,cb->prbn", cols_imag, outer_table[1], precision=lax.Precision.HIGHEST)
    odd_blocks = jnp.einsum(
        "pcrn,cb->prbn", cols_imag, outer_table[0], precision=lax.Precision.HIGHEST
    ) - jnp.einsum("pcrn,cb->prbn", cols_real, outer_table[1], precision=lax.Precision.HIGHEST)
    paired_blocks = jnp.stack([phase_blocks, odd_blocks], axis=1)
    return (paired_blocks / columns).reshape(projections, rows_local, columns)


RADIX = 8
CHUNK = 16


def split_bf16(value):
    high = value.astype(jnp.bfloat16)
    return high, (value - high.astype(jnp.float32)).astype(jnp.bfloat16)


def split_table(table):
    high = table.astype(np.float32).astype(jnp.bfloat16)
    return high, (table - high.astype(np.float64)).astype(np.float32).astype(jnp.bfloat16)


def dot_nt(left, right):
    return lax.dot_general(left, right, (((1,), (1,)), ((), ())), preferred_element_type=jnp.float32)


def dot_nn(left, right):
    return lax.dot_general(left, right, (((1,), (0,)), ((), ())), preferred_element_type=jnp.float32)


def dot3(dot, left, right):
    return dot(left[0], right[0]) + (dot(left[0], right[1]) + dot(left[1], right[0]))


def small_dft(items, sign, turn, add, sub):
    count = len(items)
    if count == 1:
        return items
    even = small_dft(items[0::2], sign, turn, add, sub)
    odd = small_dft(items[1::2], sign, turn, add, sub)
    low, high = [], []
    for k in range(count // 2):
        moved = odd[k]
        if k:
            moved = turn(moved, k, count, sign)
        low.append(add(even[k], moved))
        high.append(sub(even[k], moved))
    return low + high


def pair_turn(item, k, count, sign):
    real, imag = item
    if 4 * k == count:
        return (-imag, real) if sign > 0 else (imag, -real)
    angle = sign * 2.0 * math.pi * k / count
    cosine, sine = math.cos(angle), math.sin(angle)
    return (real * cosine - imag * sine, real * sine + imag * cosine)


def pair_add(a, b):
    return (a[0] + b[0], a[1] + b[1])


def pair_sub(a, b):
    return (a[0] - b[0], a[1] - b[1])


pair_dft = functools.partial(small_dft, turn=pair_turn, add=pair_add, sub=pair_sub)


def col_spread(x_ref, tw_ref, yh_ref, yl_ref):
    _, rows, columns = x_ref.shape
    block = columns // RADIX

    def spread(i, carry):
        at = pl.ds(pl.multiple_of(i * CHUNK, CHUNK), CHUNK)
        parts = [
            (x_ref[0, at, j * block : (j + 1) * block], x_ref[1, at, j * block : (j + 1) * block])
            for j in range(RADIX)
        ]
        for q, (real, imag) in enumerate(pair_dft(parts, -1)):
            if q:
                cosine, sine = tw_ref[q, 0:1, :], tw_ref[q, 1:2, :]
                real, imag = real * cosine + imag * sine, imag * cosine - real * sine
            for half, value in enumerate((real, imag)):
                high, low = split_bf16(value)
                yh_ref[q, at, half * block : (half + 1) * block] = high
                yl_ref[q, at, half * block : (half + 1) * block] = low
        return carry

    lax.fori_loop(0, rows // CHUNK, spread, 0)


def middle_kernel(scale, in_ref, th_ref, tl_ref, tw_ref, twc_ref, f_ref, g_ref, out_ref, yh_ref, yl_ref, t_ref):
    dists, pixes, _, width, block = in_ref.shape
    per_dist = width // CHUNK

    def spread(i, carry):
        dist = i // per_dist
        at = pl.ds(pl.multiple_of((i % per_dist) * CHUNK, CHUNK), CHUNK)
        to = pl.ds(pl.multiple_of(i * CHUNK, CHUNK), CHUNK)
        parts = [(in_ref[dist, j, 0, at, :], in_ref[dist, j, 1, at, :]) for j in range(pixes)]
        for q, (real, imag) in enumerate(pair_dft(parts, -1)):
            if q:
                cosine, sine = tw_ref[q, 0:1, :], tw_ref[q, 1:2, :]
                real, imag = real * cosine + imag * sine, imag * cosine - real * sine
            for half, value in enumerate((real, imag)):
                high, low = split_bf16(value)
                yh_ref[q, to, half * block : (half + 1) * block] = high
                yl_ref[q, to, half * block : (half + 1) * block] = low
        return carry

    lax.fori_loop(0, dists * per_dist, spread, 0)

    def transform(q, carry):
        table = (th_ref[...], tl_ref[...])
        spectrum = dot3(dot_nt, (yh_ref[q], yl_ref[q]), table)
        factors = f_ref[q]
        total_real = total_imag = bottom = None
        for dist in range(dists):
            gain = (
                factors[2 * dist : 2 * dist + 1] * g_ref[2 * dist]
                + factors[2 * dist + 1 : 2 * dist + 2] * g_ref[2 * dist + 1]
            )
            real = gain * spectrum[dist * width : (dist + 1) * width, :block]
            imag = gain * spectrum[dist * width : (dist + 1) * width, block:]
            square = gain * gain
            if dist == 0:
                total_real, total_imag, bottom = real, imag, square
            else:
                total_real, total_imag, bottom = total_real + real, total_imag + imag, bottom + square
        ratio = scale / (2.0 * (bottom + REGULARIZER))
        real, imag = total_real * ratio, total_imag * ratio
        stacked = jnp.concatenate(
            [jnp.concatenate([real, -imag], axis=1), jnp.concatenate([imag, real], axis=1)], axis=0
        )
        upper = (th_ref[:block, :], tl_ref[:block, :])
        t_ref[q] = dot3(dot_nt, upper, split_bf16(stacked))
        return carry

    lax.fori_loop(0, RADIX, transform, 0, unroll=2)

    lane = lax.broadcasted_iota(jnp.int32, (CHUNK, 2 * width), 1)
    flip = jnp.where(lane < width, -1.0, 1.0).astype(jnp.float32)

    def times_i(value):
        return pltpu.roll(value, width, 1) * flip

    def turn(value, k, count, sign):
        if 4 * k == count:
            return times_i(value)
        angle = sign * 2.0 * math.pi * k / count
        return value * math.cos(angle) + times_i(value) * math.sin(angle)

    def gather(i, carry):
        at = pl.ds(pl.multiple_of(i * CHUNK, CHUNK), CHUNK)
        twists = twc_ref[at, :]
        parts = []
        for q in range(RADIX):
            value = t_ref[q, at, :]
            if q:
                value = value * twists[:, q : q + 1] + times_i(value) * twists[:, RADIX + q : RADIX + q + 1]
            parts.append(value)
        done = small_dft(parts, 1, turn, lambda a, b: a + b, lambda a, b: a - b)
        for j in range(pixes):
            out_ref[j, at, :] = done[j]
        return carry

    lax.fori_loop(0, block // CHUNK, gather, 0)


def col_inverse_kernel(in_ref, th_ref, tl_ref, tw_ref, out_ref, ah_ref, al_ref, t_ref):
    _, per_q, rows, lanes = in_ref.shape
    block = per_q * lanes // 2

    def transform(q, carry):
        for part in range(per_q):
            high, low = split_bf16(in_ref[q, part])
            ah_ref[:, part * lanes : (part + 1) * lanes] = high
            al_ref[:, part * lanes : (part + 1) * lanes] = low
        t_ref[q] = dot3(dot_nn, (ah_ref[...], al_ref[...]), (th_ref[...], tl_ref[...]))
        return carry

    lax.fori_loop(0, RADIX, transform, 0)

    def gather(i, carry):
        at = pl.ds(pl.multiple_of(i * CHUNK, CHUNK), CHUNK)
        parts = []
        for q in range(RADIX):
            real, imag = t_ref[q, at, :block], t_ref[q, at, block:]
            if q:
                cosine, sine = tw_ref[q, 0:1, :], tw_ref[q, 1:2, :]
                real, imag = real * cosine - imag * sine, imag * cosine + real * sine
            parts.append((real, imag))
        for j, (real, imag) in enumerate(pair_dft(parts, 1)):
            out_ref[0, at, j * block : (j + 1) * block] = real
            out_ref[1, at, j * block : (j + 1) * block] = imag
        return carry

    lax.fori_loop(0, rows // CHUNK, gather, 0)


def local_copy_spec():
    return pl.BlockSpec(memory_space=pl.ANY)


def remote(src, dst, send_sem, recv_sem, device_id):
    return pltpu.make_async_remote_copy(
        src_ref=src,
        dst_ref=dst,
        send_sem=send_sem,
        recv_sem=recv_sem,
        device_id=device_id,
        device_id_type=pl.DeviceIdType.MESH,
    )


def gain_factors(defocus, rate, squared):
    envelope = jnp.exp(-rate * squared)
    angle = defocus * squared
    return envelope * jnp.sin(angle), envelope * jnp.cos(angle)


def exchange_kernel(
    dists, pixes, x_ref, th_ref, tl_ref, tw_ref, own_ref, out_ref, f_ref, g_ref,
    yh_ref, yl_ref, in_ref, held, send_sem, recv_sem, own_sem, small_send, small_recv, small_own,
):
    dist, pix = lax.axis_index("dist"), lax.axis_index("pix")
    count = dists * pixes
    me = dist * pixes + pix

    def small(step, slot):
        return remote(
            own_ref, held.at[slot], small_send.at[step], small_recv.at[step], {"dist": (dist + step) % dists}
        )

    for step in range(1, dists):
        small(step, dist).start()
    small_copy = pltpu.make_async_copy(own_ref, held.at[dist], small_own)
    small_copy.start()
    own = pltpu.make_async_copy(in_ref.at[me], out_ref.at[me], own_sem)

    def copy(step):
        target = (me + step) % count
        return remote(
            in_ref.at[target], out_ref.at[me], send_sem.at[step], recv_sem.at[step],
            {"dist": target // pixes, "pix": target % pixes},
        )

    block = x_ref.shape[2] // RADIX
    width = in_ref.shape[2]
    per_q = block // width

    def send(q):
        for part in range(per_q):
            step = (q * per_q + part + count - me) % count

            @pl.when(step != 0)
            def _():
                copy(step).start()

    def order(i):
        return (me // per_q + 1 + i) % RADIX

    col_spread(x_ref, tw_ref, yh_ref, yl_ref)

    def transform(i, carry):
        q = order(i)
        table = (th_ref[...], tl_ref[...])
        result = dot3(dot_nt, table, (yh_ref[q], yl_ref[q]))
        for part in range(per_q):
            for half in range(2):
                first = half * block + part * width
                in_ref[q * per_q + part, half] = result[first : first + width]

        @pl.when(i > 0)
        def _():
            send(order(i + RADIX - 1))

        return carry

    def finish(step, carry):
        copy(step).wait_send()
        source = (me + count - step) % count
        remote(
            in_ref.at[source], out_ref.at[source], send_sem.at[step], recv_sem.at[step],
            {"dist": source // pixes, "pix": source % pixes},
        ).wait_recv()
        return carry

    lax.fori_loop(0, RADIX, transform, 0)

    for step in range(1, dists):
        small(step, dist).wait_send()
        small(step, (dist + dists - step) % dists).wait_recv()
    small_copy.wait()
    send(order(RADIX - 1))
    own.start()
    radix = RADIX
    row_freq = radix * lax.broadcasted_iota(jnp.int32, (radix, block), 1) + lax.broadcasted_iota(
        jnp.int32, (radix, block), 0
    )
    row_squared = signed_square(row_freq, radix * block)
    first = me * width
    col_freq = radix * (first % block + lax.broadcasted_iota(jnp.int32, (width, block), 0)) + first // block
    col_squared = signed_square(col_freq, radix * block)
    for d in range(dists):
        defocus, rate = held[d, 0:1, 0:1], held[d, 1:2, 0:1]
        sine, cosine = gain_factors(defocus, rate, row_squared)
        f_ref[:, 2 * d, :] = sine
        f_ref[:, 2 * d + 1, :] = cosine
        sine, cosine = gain_factors(defocus, rate, col_squared)
        g_ref[2 * d] = cosine - ABSORB_RATIO * sine
        g_ref[2 * d + 1] = sine + ABSORB_RATIO * cosine

    lax.fori_loop(1, count, finish, 0)
    own.wait()


def exchange(dists, pixes, images, th, tl, tw, own):
    count = dists * pixes
    _, rows, columns = images.shape
    width = columns // count
    return pl.pallas_call(
        functools.partial(exchange_kernel, dists, pixes),
        out_shape=(
            jax.ShapeDtypeStruct((count, 2, width, rows), jnp.float32),
            jax.ShapeDtypeStruct((RADIX, 2 * dists, rows), jnp.float32),
            jax.ShapeDtypeStruct((2 * dists, width, rows), jnp.float32),
        ),
        in_specs=[pl.BlockSpec(memory_space=pltpu.VMEM)] * 5,
        out_specs=(local_copy_spec(),) + (pl.BlockSpec(memory_space=pltpu.VMEM),) * 2,
        scratch_shapes=[
            pltpu.VMEM((RADIX, rows, 2 * columns // RADIX), jnp.bfloat16),
            pltpu.VMEM((RADIX, rows, 2 * columns // RADIX), jnp.bfloat16),
            pltpu.VMEM((count, 2, width, rows), jnp.float32),
            pltpu.VMEM((dists,) + own.shape, jnp.float32),
            pltpu.SemaphoreType.DMA((count,)),
            pltpu.SemaphoreType.DMA((count,)),
            pltpu.SemaphoreType.DMA,
            pltpu.SemaphoreType.DMA((dists,)),
            pltpu.SemaphoreType.DMA((dists,)),
            pltpu.SemaphoreType.DMA,
        ],
        compiler_params=pltpu.CompilerParams(has_side_effects=True),
    )(images, th, tl, tw, own)


RELAY_LAG = 1


def relay_kernel(pixes, in_ref, out_ref, send_sem, recv_sem, hop_send, hop_recv, own_sem):
    dist, pix = lax.axis_index("dist"), lax.axis_index("pix")
    mate = dist + 1 - 2 * (dist % 2)
    across = (dist + 2) % 4
    corner = (mate + 2) % 4

    def first(step, source):
        target = (pix + step) % pixes
        return remote(
            in_ref.at[target], out_ref.at[dist, source], send_sem.at[step], recv_sem.at[step], {"pix": target}
        )

    def source_of(step):
        return (pix + pixes - step) % pixes

    def hop(owner, step, kind, target):
        block = out_ref.at[owner, source_of(step)]
        begin = in_ref.at[pix] if step == 0 and kind < 2 else block
        return remote(begin, block, hop_send.at[kind, step], hop_recv.at[kind, step], {"dist": target})

    own = pltpu.make_async_copy(in_ref.at[pix], out_ref.at[dist, pix], own_sem)
    own.start()
    for step in range(1, pixes):
        first(step, pix).start()

    def relay(step):
        hop(across, step, 0, across).wait_recv()
        hop(across, step, 2, mate).start()

    for step in range(pixes):
        if step:
            first(step, source_of(step)).wait_recv()
        hop(dist, step, 0, across).start()
        hop(dist, step, 1, mate).start()
        if step >= RELAY_LAG:
            relay(step - RELAY_LAG)
    for step in range(pixes - RELAY_LAG, pixes):
        relay(step)
    own.wait()
    for step in range(pixes):
        if step:
            first(step, pix).wait_send()
        hop(dist, step, 0, across).wait_send()
        hop(dist, step, 1, mate).wait_send()
        hop(mate, step, 1, mate).wait_recv()
        hop(across, step, 2, mate).wait_send()
        hop(corner, step, 2, mate).wait_recv()


def relay_all(dists, pixes, array):
    return pl.pallas_call(
        functools.partial(relay_kernel, pixes),
        out_shape=jax.ShapeDtypeStruct((dists,) + array.shape, array.dtype),
        in_specs=[local_copy_spec()],
        out_specs=local_copy_spec(),
        scratch_shapes=[
            pltpu.SemaphoreType.DMA((pixes,)),
            pltpu.SemaphoreType.DMA((pixes,)),
            pltpu.SemaphoreType.DMA((3, pixes)),
            pltpu.SemaphoreType.DMA((3, pixes)),
            pltpu.SemaphoreType.DMA,
        ],
        compiler_params=pltpu.CompilerParams(has_side_effects=True),
    )(array)


def vmem_call(kernel, out_shape, scratch, *args):
    return pl.pallas_call(
        kernel,
        out_shape=jax.ShapeDtypeStruct(out_shape, jnp.float32),
        in_specs=[pl.BlockSpec(memory_space=pltpu.VMEM)] * len(args),
        out_specs=pl.BlockSpec(memory_space=pltpu.VMEM),
        scratch_shapes=scratch,
    )(*args)


def fast_body(contrast, defocus, blurring):
    images = contrast[0]
    _, rows, columns = images.shape
    pixes, dists = lax.axis_size("pix"), lax.axis_size("dist")
    count = pixes * dists
    block = columns // RADIX
    width = columns // count
    per_q = block // width
    total_rows = rows * pixes

    turns = np.outer(np.arange(block), np.arange(block)) % block * (2.0 * np.pi / block)
    cosine, sine = np.cos(turns), np.sin(turns)
    table = np.block([[cosine, sine], [-sine, cosine]])
    order = np.concatenate(
        [np.arange(width) + part * width + half * block for part in range(per_q) for half in range(2)]
    )
    th, tl = split_table(table)
    ph, pl_ = split_table(table[order])
    twist = np.outer(np.arange(RADIX), np.arange(block)) * (2.0 * np.pi / columns)
    tw = np.stack([np.cos(twist), np.sin(twist)], axis=1).astype(np.float32)
    twc = np.concatenate([np.cos(twist).T, np.sin(twist).T], axis=1).astype(np.float32)

    own = jnp.broadcast_to(jnp.concatenate([defocus, blurring] * 4)[:, None], (8, 128))

    received, f_table, g_table = exchange(dists, pixes, images, th, tl, tw, own)
    back = vmem_call(
        functools.partial(middle_kernel, 1.0 / (total_rows * columns)),
        (pixes, rows, 2 * width),
        [pltpu.VMEM((RADIX, dists * width, 2 * rows), jnp.bfloat16)] * 2
        + [pltpu.VMEM((RADIX, rows, 2 * width), jnp.float32)],
        received.reshape(dists, pixes, 2, width, rows), th, tl, tw, twc, f_table, g_table,
    )
    arrived = relay_all(dists, pixes, back)
    return vmem_call(
        col_inverse_kernel,
        (2, rows, columns),
        [pltpu.VMEM((rows, 2 * block), jnp.bfloat16)] * 2
        + [pltpu.VMEM((RADIX, rows, 2 * block), jnp.float32)],
        arrived.reshape(RADIX, per_q, rows, 2 * width), ph, pl_, tw,
    )


def body(contrast, defocus, blurring):
    _, projections, rows, columns = contrast.shape
    pixes, dists = lax.axis_size("pix"), lax.axis_size("dist")
    fits = (
        projections == 2
        and pixes == RADIX
        and dists == 4
        and rows * pixes == columns
        and columns % (dists * pixes * 64) == 0
        and columns // (dists * pixes) == rows // dists == 64
    )
    return (fast_body if fits else general_body)(contrast, defocus, blurring)


def solution(mesh):
    return jax.shard_map(
        body,
        mesh=mesh,
        in_specs=(P("dist", None, "pix", None), P("dist"), P("dist")),
        out_specs=P(None, "pix", None),
        check_vma=False,
    )
```
